32 devices in a mesh: dp: 8 (over y, x, core), tensor: 4 (over z).
Axes of the slice: x: 2, y: 2, z: 4, core: 2. Of those that a mesh axis runs over, the one named last changes fastest.
Arguments:
- layer_input: bfloat16 [16384, 4096], P('dp', 'tensor'), may hold values from -54 to 54
- queries: bfloat16 [16384, 2048], P('dp', 'tensor'), may hold values from -6 to 6
- keys_values: bfloat16 [16384, 2, 1024], P('dp', None, 'tensor'), may hold values from -6 to 6
- out_grads: bfloat16 [16384, 2048], P('dp', 'tensor'), may hold values from -6 to 6
- log_sums: bfloat16 [16384, 16], P('dp', 'tensor'), may hold values from 2.5 to 5.5
- deltas: bfloat16 [16384, 16], P('dp', 'tensor'), may hold values from -1.5 to 1.5
- tile_fill: int32 [8, 16], replicated, may hold values from 1 to 128, as said below
- tile_cont: int32 [8, 16], replicated, may hold values from 0 to 1, as said below
- moment_first: float32 [4096, 2, 1024], P(('tensor', 'dp')), may hold values from -2 to 2
- moment_second: float32 [2, 8], replicated, may hold values from 0.05 to 0.5
Outputs:
- update: float32 [4096, 2, 1024], P(('tensor', 'dp'))
- new_first: float32 [4096, 2, 1024], P(('tensor', 'dp'))
- new_second: float32 [2, 8], replicated
The draws below stay inside these ranges and needn't reach their ends.
Inputs may be any that keep to these rules, and one draw needn't show every extreme that they name: `tile_fill`: a tile followed by a tile with tile_cont 1 has all 128 positions live. Documents span one or two tiles: tile_cont is 0 for the first tile of each group and never 1 for two tiles in a row.
All inputs are finite; a program needn't handle non-finite values.
Results may differ from the reference program's by a relative error of at most 0.0055.
Values may be sent and summed in bfloat16 or wider, within the bound.
A program may use at most 64 MiB of HBM per device.

```python
import math
import jax
import jax.numpy as jnp
from jax import lax

D = 4096
HQ = 16
HK = 8
HD = 128
BLK = 128
TILES_DEV = 16
TOKENS = 16384
N_DP = 8


def tile_layout(key):
    key = jax.random.fold_in(key, 7)
    key_bits, key_fill = jax.random.split(key)
    coin_bits = jax.random.randint(key_bits, (N_DP, TILES_DEV), 0, 2)
    tile_index = jnp.arange(TILES_DEV)

    def advance(previous, column):
        col_bits, position = column
        linked = jnp.where(position == 1, 1, jnp.where(position == 0, 0, col_bits * (1 - previous)))
        linked = linked.astype(jnp.int32)
        return (linked, linked)
    final_state, linked = lax.scan(advance, jnp.zeros((N_DP,), jnp.int32), (coin_bits.T, tile_index))
    tile_cont = linked.T.astype(jnp.int32)
    following = jnp.concatenate([tile_cont[:, 1:], jnp.zeros_like(tile_cont[:, :1])], 1)
    raw_fill = jax.random.randint(key_fill, (N_DP, TILES_DEV), 1, BLK + 1)
    tile_fill = jnp.where(following == 1, BLK, raw_fill).astype(jnp.int32)
    return (tile_fill, tile_cont)


def draw_tile_fill(key, part):
    return tile_layout(key)[0]


def draw_tile_cont(key, part):
    return tile_layout(key)[1]


def draw_layer_input(key, part):
    key = jax.random.fold_in(key, 11)
    key_cols, key_vals = jax.random.split(key, 2)
    columns = jnp.arange(D, dtype=jnp.float32) / D
    spread = jnp.exp(jax.random.uniform(key_cols, (D,), jnp.float32, math.log(0.3), math.log(3.0)))
    col_ramp = 1.0 + 2.0 * columns
    base_vals = jnp.clip(jax.random.normal(key_vals, (TOKENS, D), jnp.float32), -6.0, 6.0)
    return (base_vals * spread[None, :] * col_ramp[None, :]).astype(jnp.bfloat16)


def steps_of(rng, extent, shards, smallest, largest):
    gain, own = 1.0, jax.random.fold_in(rng, 6)
    for dim, shards_of in shards:
        draws = jnp.exp(jax.random.uniform(jax.random.fold_in(own, dim), (shards_of,), jnp.float32, smallest / len(shards), largest / len(shards)))
        gain = gain * jnp.repeat(draws, extent[dim] // shards_of).reshape([-1 if axis == dim else 1 for axis in range(len(extent))])
    return gain


def scatter_about(own_key, shape, scale, reach, pieces=(), held_as=jnp.bfloat16):
    drawn = jax.random.normal(own_key, shape, jnp.float32) * scale
    if len(pieces) > 0:
        drawn = steps_of(own_key, shape, pieces, -0.22, 0.18) * drawn
    return jnp.clip(drawn, min=-reach, max=reach).astype(held_as)


def setup_inputs(seed: int = 0) -> dict:
    arg_keys = jax.random.split(jax.random.key(seed), 11)
    layer_input = draw_layer_input(jax.random.fold_in(arg_keys[10], 71), 0)
    queries = scatter_about(arg_keys[1], (TOKENS, HQ * HD), 1.0, 6.0, ((0, 8), (1, 4)))
    keys_values = scatter_about(arg_keys[2], (TOKENS, 2, HK * HD), 1.0, 6.0, ((0, 8), (2, 4)))
    out_grads = scatter_about(arg_keys[3], (TOKENS, HQ * HD), 1.0, 6.0, ((0, 8), (1, 4)))
    log_sums = jnp.clip(2.5 + 3.0 * jax.random.uniform(arg_keys[4], (TOKENS, HQ), jnp.float32) ** steps_of(arg_keys[4], (TOKENS, HQ), ((0, 8), (1, 4)), -0.2, 0.2), 2.5, 5.5).astype(jnp.bfloat16)
    deltas = scatter_about(arg_keys[5], (TOKENS, HQ), 0.3, 1.5, ((0, 8), (1, 4)))
    tile_fill = draw_tile_fill(jax.random.fold_in(arg_keys[10], 71), 0)
    tile_cont = draw_tile_cont(jax.random.fold_in(arg_keys[10], 71), 0)
    moment_first = scatter_about(arg_keys[8], (D, 2, HK * HD), 0.3, 2.0, ((0, 32),), jnp.float32)
    moment_second = jnp.clip(jnp.exp(jax.random.uniform(arg_keys[9], (2, HK), jnp.float32, math.log(0.05), math.log(0.5))), 0.05, 0.5)
    return {"layer_input": layer_input, "queries": queries, "keys_values": keys_values, "out_grads": out_grads, "log_sums": log_sums, "deltas": deltas, "tile_fill": tile_fill, "tile_cont": tile_cont, "moment_first": moment_first, "moment_second": moment_second}


HIGHEST_PRECISION = lax.Precision.HIGHEST

def band_grads(q_tiles, k_tiles, v_tiles, do_tiles, lse_tiles, delta_tiles, fill_tiles, cont_tiles):
    tile_total, block_len, groups, head_width = q_tiles.shape
    scale_qk = head_width ** (-0.5)
    q_full = q_tiles.astype(jnp.float32)
    do_full = do_tiles.astype(jnp.float32)
    k_full = k_tiles.astype(jnp.float32)
    v_full = v_tiles.astype(jnp.float32)
    zero_tile = jnp.zeros_like(k_full[:1])
    k_window = jnp.concatenate([jnp.concatenate([zero_tile, k_full[:-1]], 0), k_full], 1)
    v_window = jnp.concatenate([jnp.concatenate([zero_tile, v_full[:-1]], 0), v_full], 1)
    places = jnp.arange(block_len)
    live_rows = places[None, :] < fill_tiles[:, None]
    causal = places[:, None] >= places[None, :]
    own_part = live_rows[:, :, None] & causal[None]
    prev_part = live_rows[:, :, None] & (cont_tiles[:, None, None] == 1) & (places[None, None, :] >= 0)
    allowed = jnp.concatenate([prev_part, own_part], 2)[:, None]
    scores = jnp.einsum('sqgd,skd->sgqk', q_full, k_window, precision=HIGHEST_PRECISION) * scale_qk
    lse_rows = jnp.swapaxes(lse_tiles.astype(jnp.float32), 1, 2)[..., None]
    delta_rows = jnp.swapaxes(delta_tiles.astype(jnp.float32), 1, 2)[..., None]
    prob_vals = jnp.where(allowed, jnp.exp(scores - lse_rows), 0.0)
    dprobs = jnp.einsum('sqgd,skd->sgqk', do_full, v_window, precision=HIGHEST_PRECISION)
    dscores = prob_vals * (dprobs - delta_rows)
    prob_half = lax.optimization_barrier(prob_vals.astype(jnp.bfloat16)).astype(jnp.float32)
    score_half = lax.optimization_barrier(dscores.astype(jnp.bfloat16)).astype(jnp.float32)
    value_grad = jnp.einsum('sgqk,sqgd->skd', prob_half, do_full, precision=HIGHEST_PRECISION)
    key_grad = jnp.einsum('sgqk,sqgd->skd', score_half, q_full, precision=HIGHEST_PRECISION) * scale_qk
    key_out = key_grad[:, block_len:] + jnp.concatenate([key_grad[1:, :block_len], jnp.zeros_like(key_grad[:1, :block_len])], 0)
    value_out = value_grad[:, block_len:] + jnp.concatenate([value_grad[1:, :block_len], jnp.zeros_like(value_grad[:1, :block_len])], 0)
    return (key_out, value_out)

def reference(layer_input, queries, keys_values, out_grads, log_sums, deltas, tile_fill, tile_cont, moment_first, moment_second):
    tiles_all = N_DP * TILES_DEV
    groups = HQ // HK
    q_heads = queries.reshape(tiles_all, BLK, HK, groups, HD).transpose(2, 0, 1, 3, 4)
    do_heads = out_grads.reshape(tiles_all, BLK, HK, groups, HD).transpose(2, 0, 1, 3, 4)
    k_heads = keys_values[:, 0].reshape(tiles_all, BLK, HK, HD).transpose(2, 0, 1, 3)
    v_heads = keys_values[:, 1].reshape(tiles_all, BLK, HK, HD).transpose(2, 0, 1, 3)
    lse_heads = log_sums.reshape(tiles_all, BLK, HK, groups).transpose(2, 0, 1, 3)
    delta_heads = deltas.reshape(tiles_all, BLK, HK, groups).transpose(2, 0, 1, 3)
    fill_flat = tile_fill.reshape(-1)
    cont_flat = tile_cont.reshape(-1)

    def one_head(operands):
        q_one, k_one, v_one, do_one, lse_one, delta_one = operands
        key_out, value_out = band_grads(q_one, k_one, v_one, do_one, lse_one, delta_one, fill_flat, cont_flat)
        return jnp.stack([key_out, value_out], 2).astype(jnp.bfloat16)
    per_head = lax.map(one_head, (q_heads, k_heads, v_heads, do_heads, lse_heads, delta_heads))
    kv_grads = per_head.transpose(1, 2, 3, 0, 4).reshape(TOKENS, 2 * HK * HD)
    summed = lax.dot_general(layer_input, kv_grads, (((0,), (0,)), ((), ())), preferred_element_type=jnp.float32)
    proj_grads = summed.reshape(D, 2, HK * HD) / math.sqrt(TOKENS)
    new_first = 0.9 * moment_first + (1 - 0.9) * proj_grads
    squares = lax.optimization_barrier(jnp.sum(jnp.square(proj_grads).reshape(D, 2, HK, HD), axis=(0, 3)))
    new_second = 0.95 * moment_second + (1 - 0.95) * squares / (D * HD)
    step_size = jnp.sqrt(new_second / (1 - 0.95 ** 2)) + 1e-08
    update = ((new_first / (1 - 0.9 ** 2)).reshape(D, 2, HK, HD) / step_size[None, :, :, None]).reshape(D, 2, HK * HD)
    return (update, new_first, new_second)
```

```python
import functools
import math

import jax
import jax.numpy as jnp
from jax import lax
from jax.experimental import pallas as pl
from jax.experimental.pallas import tpu as pltpu
from jax.sharding import PartitionSpec as P

D = 4096
HD = 128

ADAM_ONE = 0.9
ADAM_TWO = 0.95
ADAM_EPS = 1e-08
MESH = pl.DeviceIdType.MESH
NT = (((1,), (1,)), ((), ()))


def attend_kernel(tiles, group_size, fill_ref, cont_ref, q_ref, k_ref, v_ref, do_ref, lse_ref, delta_ref, out_ref):
    group = lax.axis_index("dp")
    block = k_ref.shape[0] // tiles
    scale_qk = HD ** (-0.5)
    wide = 2 * group_size * block
    key_place = lax.broadcasted_iota(jnp.int32, (block, wide), 0)
    column = lax.broadcasted_iota(jnp.int32, (block, wide), 1)
    query_place = column % block
    is_next = column >= group_size * block

    def one_tile(tile, carry):
        after = jnp.minimum(tile + 1, tiles - 1)
        here = pl.ds(pl.multiple_of(tile * block, block), block)
        there = pl.ds(pl.multiple_of(after * block, block), block)
        fill_here = fill_ref[group, tile]
        fill_there = jnp.where(tile + 1 < tiles, fill_ref[group, after] * (cont_ref[group, after] == 1).astype(jnp.int32), 0)
        heads = [slice(h * HD, (h + 1) * HD) for h in range(group_size)]
        q_cat = jnp.concatenate([q_ref[w, h] for w in (here, there) for h in heads], 0)
        do_cat = jnp.concatenate([do_ref[w, h] for w in (here, there) for h in heads], 0)
        lse = jnp.concatenate([lse_ref[0, h : h + 1, w] for w in (here, there) for h in range(group_size)], 1)
        delta = jnp.concatenate([delta_ref[0, h : h + 1, w] for w in (here, there) for h in range(group_size)], 1)
        scores = lax.dot_general(k_ref[here, :], q_cat, NT, preferred_element_type=jnp.float32) * scale_qk
        limit = jnp.where(is_next, fill_there, fill_here)
        allowed = (query_place < limit) & (is_next | (query_place >= key_place))
        prob = jnp.where(allowed, jnp.exp(scores - lse), 0.0)
        dprob = lax.dot_general(v_ref[here, :], do_cat, NT, preferred_element_type=jnp.float32)
        dscore = prob * (dprob - delta)
        value_grad = jnp.dot(prob.astype(jnp.bfloat16), do_cat, preferred_element_type=jnp.float32)
        key_grad = jnp.dot(dscore.astype(jnp.bfloat16), q_cat, preferred_element_type=jnp.float32) * scale_qk
        out_ref[0, here, :] = key_grad.astype(jnp.bfloat16)
        out_ref[1, here, :] = value_grad.astype(jnp.bfloat16)
        return carry

    lax.fori_loop(0, tiles, one_tile, 0, unroll=2)


def attend(queries, keys, values, out_grads, lse_rows, delta_rows, tile_fill, tile_cont):
    tokens = queries.shape[0]
    kv_local = keys.shape[1] // HD
    group_size = queries.shape[1] // keys.shape[1]
    tiles = tile_fill.shape[1]
    smem = pl.BlockSpec(memory_space=pltpu.SMEM)
    q_spec = pl.BlockSpec((tokens, group_size * HD), lambda h: (0, h))
    k_spec = pl.BlockSpec((tokens, HD), lambda h: (0, h))
    row_spec = pl.BlockSpec((1, group_size, tokens), lambda h: (h, 0, 0))
    return pl.pallas_call(
        functools.partial(attend_kernel, tiles, group_size),
        grid=(kv_local,),
        out_shape=jax.ShapeDtypeStruct((2 * kv_local, tokens, HD), jnp.bfloat16),
        in_specs=[smem, smem, q_spec, k_spec, k_spec, q_spec, row_spec, row_spec],
        out_specs=pl.BlockSpec((2, tokens, HD), lambda h: (h, 0, 0)),
        compiler_params=pltpu.CompilerParams(vmem_limit_bytes=32 * 2**20),
    )(tile_fill, tile_cont, queries, keys, values, out_grads, lse_rows, delta_rows)


def token_split(tokens, planes):
    if planes < 4 or tokens < 1024:
        return tokens
    return tokens - tokens * 3 // 8 // 128 * 128


def sum_kernel(
    groups, planes, split, inv, kv_ref, layer_ref, out_ref, sq_ref,
    layer, flipped, gathered, lent, lent_flipped, keep, pair_send, pair_recv, chip_send, chip_recv,
    part_send, part_recv, squares, sq_all,
    load_sem, own_sem, kv_right, kv_left, kv_recv, lent_ssem, lent_rsem, pair_ssem, pair_rsem, chip_ssem, chip_rsem,
    part_ssem, part_rsem, sq_ssem, sq_rsem,
):
    me, plane = lax.axis_index("dp"), lax.axis_index("tensor")
    chips = groups // 2
    chip, core = me // 2, me % 2
    partner = me + 1 - 2 * core
    chunks, tokens, _ = kv_ref.shape
    rows = layer_ref.shape[1]
    rows_out = rows // groups
    half = rows // 2
    events = planes * chunks
    lending = split < tokens
    is_end = (plane == 0) | (plane == planes - 1)
    is_helper = (plane == 1) | (plane == planes - 2)
    helped = jnp.where(plane == 1, 0, planes - 1)
    helper = jnp.where(plane == 0, 1, planes - 2)
    mid = split // 256 * 128
    segments = ((split, tokens - split), (0, mid), (mid, split - mid)) if lending else ((0, mid), (mid, split - mid))

    load = pltpu.make_async_copy(layer_ref, layer, load_sem)
    load.start()
    own = [pltpu.make_async_copy(kv_ref.at[c], gathered.at[c, plane], own_sem.at[c]) for c in range(chunks)]
    for c in range(chunks):
        own[c].start()

    barrier = pltpu.get_barrier_semaphore()
    mine = me * planes + plane

    def greet(step, carry):
        other = lax.rem(mine + step, groups * planes)
        pl.semaphore_signal(barrier, inc=1, device_id=(other // planes, other % planes), device_id_type=MESH)
        return carry

    lax.fori_loop(1, groups * planes, greet, 0)
    pl.semaphore_wait(barrier, groups * planes - 1)

    far = jnp.where(plane < planes // 2, 1, -1)
    near_count = jnp.minimum(plane, planes - 1 - plane)

    def piece_of(w):
        turn = (w + 1) // 2
        swing = jnp.where(w % 2 == 1, turn, -turn)
        return plane + far * jnp.where(w <= 2 * near_count, swing, w - near_count)

    def turn_of(e):
        k = e - 2 * chunks
        last, odd = k == 2 * chunks - 1, k % 2 == 1
        mixed = (planes >= 4) & (k >= 0) & (k < 2 * chunks)
        w = jnp.where(last | (jnp.logical_not(odd) & (k > 0)), 3, 2)
        c = jnp.where(last, chunks - 1, jnp.where(odd, (k + 1) // 2, jnp.maximum(k // 2 - 1, 0)))
        return jnp.where(mixed, w, e // chunks), jnp.where(mixed, c, e % chunks)

    def place(e):
        w, c = turn_of(e)
        return c, piece_of(w)

    def lend_copy():
        return pltpu.make_async_remote_copy(
            src_ref=layer_ref.at[pl.ds(split, tokens - split), :], dst_ref=lent, send_sem=lent_ssem,
            recv_sem=lent_rsem, device_id=(me, helper), device_id_type=MESH,
        )

    def move(c, p, s, right):
        start, size = segments[s]
        where = gathered.at[c, p, pl.ds(start, size)]
        to = jnp.minimum(plane + 1, planes - 1) if right else jnp.maximum(plane - 1, 0)
        return pltpu.make_async_remote_copy(
            src_ref=where, dst_ref=where, send_sem=(kv_right if right else kv_left).at[c, p, s],
            recv_sem=kv_recv.at[c, p, s], device_id=(me, to), device_id_type=MESH,
        )

    def passes(p, s, right):
        lent_part = lending and s == 0
        if right:
            there = plane < planes - 2 if lent_part else plane < planes - 1
            return (p <= plane) & there
        there = plane > 1 if lent_part else plane > 0
        return (p >= plane) & there

    def pass_on(c, p, s):
        for right in (True, False):
            @pl.when(passes(p, s, right))
            def _():
                move(c, p, s, right).start()

    def arrive(c, p, s):
        if lending and s == 0:
            @pl.when(jnp.logical_not(is_end))
            def _():
                move(c, p, s, True).wait_recv()
        else:
            move(c, p, s, True).wait_recv()

    row_block = min(256, half)

    def multiply(source, lhs_from, rhs_from, length, c, p, job):
        weights = (c, p, pl.ds(rhs_from, length))

        def sent(i, carry):
            at = pl.multiple_of(i * row_block, row_block)
            pair_send[job, pl.ds(at, row_block), :] = jnp.dot(
                source[pl.ds(half + at, row_block), pl.ds(lhs_from, length)], gathered[weights],
                preferred_element_type=jnp.float32,
            ).astype(jnp.bfloat16)
            return carry

        def kept(i, carry):
            at = pl.multiple_of(i * row_block, row_block)
            keep[job, pl.ds(at, row_block), :] = jnp.dot(
                source[pl.ds(at, row_block), pl.ds(lhs_from, length)], gathered[weights],
                preferred_element_type=jnp.float32,
            )
            return carry

        lax.fori_loop(0, half // row_block, sent, 0)
        pair_copy(job).start()
        lax.fori_loop(0, half // row_block, kept, 0)

    def slice_of(k):
        return pl.ds(pl.multiple_of(k * rows_out, rows_out), rows_out)

    def pair_copy(job):
        return pltpu.make_async_remote_copy(
            src_ref=pair_send.at[job], dst_ref=pair_recv.at[job], send_sem=pair_ssem.at[job],
            recv_sem=pair_rsem.at[job], device_id=(partner, plane), device_id_type=MESH,
        )

    def chip_copy(job, step):
        other = lax.rem(chip + step, chips)
        return pltpu.make_async_remote_copy(
            src_ref=chip_send.at[job, step - 1], dst_ref=chip_recv.at[job, step - 1],
            send_sem=chip_ssem.at[job, step - 1], recv_sem=chip_rsem.at[job, step - 1],
            device_id=(2 * other + core, plane), device_id_type=MESH,
        )

    def part_copy(c, p):
        return pltpu.make_async_remote_copy(
            src_ref=part_send.at[c, p], dst_ref=part_recv.at[c, p], send_sem=part_ssem.at[c, p],
            recv_sem=part_rsem.at[c, p], device_id=(me, helped), device_id_type=MESH,
        )

    def own_job(c, p):
        return c * planes + p

    def part_job(c, p):
        return events + c * planes + p

    def scatter(job):
        pair_copy(job).wait_recv()
        for step in range(1, chips):
            other = slice_of(lax.rem(chip + step, chips))
            both = keep[job, other, :] + pair_recv[job, other, :].astype(jnp.float32)
            chip_send[job, step - 1] = both.astype(jnp.bfloat16)
            chip_copy(job, step).start()

    def total_of(job):
        mine = slice_of(chip)
        total = keep[job, mine, :] + pair_recv[job, mine, :].astype(jnp.float32)
        for step in range(1, chips):
            chip_copy(job, step).wait_recv()
            total = total + chip_recv[job, step - 1].astype(jnp.float32)
        return total

    def finish(c, p, total):
        total = total * inv
        out_ref[c, p] = total
        squares[pl.ds(c * planes + p, 1), :] = jnp.sum(total * total, axis=0, keepdims=True)

    def helped_total(c, p, total):
        part_copy(c, p).wait_recv()
        return total + part_recv[c, p].astype(jnp.float32)

    def gather_own(e):
        w, c = turn_of(e)
        p = piece_of(w)
        total = total_of(own_job(c, p))
        if not lending:
            finish(c, p, total)
            return
        plain = jnp.logical_not(is_end) | (w == 0)

        @pl.when(plain)
        def _():
            finish(c, p, total)

        @pl.when(is_end & (w >= 3))
        def _():
            finish(c, p, helped_total(c, p, total))

        @pl.when(is_end & ((w == 1) | (w == 2)))
        def _():
            out_ref[c, p] = total

    def late_finish(e):
        turn, c = turn_of(e)

        @pl.when(is_end & (turn == 3))
        def _():
            for w in (1, 2):
                p = piece_of(w)
                finish(c, p, helped_total(c, p, out_ref[c, p]))

    def for_parts(e, act):
        w, c = turn_of(e)

        @pl.when(is_helper & (w == 2))
        def _():
            def both(i, carry):
                act(c, piece_of(i))
                return carry

            lax.fori_loop(0, 2, both, 0)

        @pl.when(is_helper & (w >= 3))
        def _():
            act(c, piece_of(w))

    def part_multiply(c, p):
        multiply(lent_flipped, 0, split, tokens - split, c, p, part_job(c, p))

    def part_scatter(c, p):
        scatter(part_job(c, p))

    def part_gather(c, p):
        part_send[c, p] = total_of(part_job(c, p)).astype(jnp.bfloat16)
        part_copy(c, p).start()

    unit = min(128, rows_out)
    flip_block = 128

    def flip(source, target, i, carry):
        turned = source[:, pl.ds(pl.multiple_of(i * flip_block, flip_block), flip_block)].T
        for sub in range(flip_block // unit):
            start = i * flip_block + sub * unit
            piece = start // rows_out
            owner = piece // 2 + jnp.where(piece % 2 == core, 0, chips)
            to = pl.multiple_of(owner * rows_out + start % rows_out, unit)
            target[pl.ds(to, unit), :] = turned[sub * unit : (sub + 1) * unit]
        return carry

    if lending:
        @pl.when(is_end)
        def _():
            lend_copy().start()

    for c in range(chunks):
        own[c].wait()
        for s in range(len(segments)):
            pass_on(c, plane, s)

    load.wait()
    lax.fori_loop(0, rows // flip_block, functools.partial(flip, layer, flipped), 0)

    def one_event(e, carry):
        w, c = turn_of(e)
        p = piece_of(w)

        @pl.when(w > 0)
        def _():
            for s in range(len(segments)):
                arrive(c, p, s)
                pass_on(c, p, s)

        if lending:
            @pl.when(is_helper & (e == 2 * chunks))
            def _():
                lend_copy().wait_recv()
                lax.fori_loop(0, rows // flip_block, functools.partial(flip, lent, lent_flipped), 0)

            for_parts(e, part_multiply)
            short = is_end & (w > 0)

            @pl.when(short)
            def _():
                multiply(flipped, 0, 0, split, c, p, own_job(c, p))

            @pl.when(jnp.logical_not(short))
            def _():
                multiply(flipped, 0, 0, tokens, c, p, own_job(c, p))
        else:
            multiply(flipped, 0, 0, tokens, c, p, own_job(c, p))

        @pl.when(e >= 1)
        def _():
            if lending:
                for_parts(e - 1, part_scatter)
            scatter(own_job(*place(e - 1)))

        @pl.when(e >= 2)
        def _():
            if lending:
                for_parts(e - 2, part_gather)
            gather_own(e - 2)

        if lending:
            late_finish(e)
        return carry

    lax.fori_loop(0, events, one_event, 0)
    if lending:
        for_parts(events - 1, part_scatter)
    scatter(own_job(*place(events - 1)))
    if lending:
        for_parts(events - 2, part_gather)
        for_parts(events - 1, part_gather)
    gather_own(events - 2)
    gather_own(events - 1)

    lane_sums = jnp.sum(squares[...], axis=1, keepdims=True)
    row = lax.broadcasted_iota(jnp.int32, (squares.shape[0], HD), 0)
    lane = lax.broadcasted_iota(jnp.int32, (squares.shape[0], HD), 1)
    sq_all[mine] = jnp.sum(jnp.where(row == lane, lane_sums, 0.0), axis=0, keepdims=True)

    def sq_copy(step):
        other = lax.rem(mine + step, groups * planes)
        return pltpu.make_async_remote_copy(
            src_ref=sq_all.at[mine], dst_ref=sq_all.at[mine], send_sem=sq_ssem, recv_sem=sq_rsem,
            device_id=(other // planes, other % planes), device_id_type=MESH,
        )

    def send_squares(step, carry):
        sq_copy(step).start()
        return carry

    lax.fori_loop(1, groups * planes, send_squares, 0)
    others = sq_all.at[pl.ds(0, groups * planes - 1)]
    pltpu.make_async_copy(others, others, sq_rsem).wait()
    sq_ref[...] = jnp.sum(sq_all[...], axis=0)
    pltpu.make_async_copy(others, others, sq_ssem).wait()

    if lending:
        @pl.when(is_end)
        def _():
            lend_copy().wait_send()

    def drain_job(job):
        pair_copy(job).wait_send()
        for step in range(1, chips):
            chip_copy(job, step).wait_send()

    def drain(e, carry):
        c, p = e // planes, e % planes
        drain_job(own_job(c, p))
        if lending:
            @pl.when(is_helper & (p != helped))
            def _():
                drain_job(part_job(c, p))
                part_copy(c, p).wait_send()

        for s in range(len(segments)):
            for right in (True, False):
                @pl.when(passes(p, s, right))
                def _():
                    move(c, p, s, right).wait_send()
        return carry

    lax.fori_loop(0, events, drain, 0)


def sum_over_groups(kv_chunks, layer_input, groups, planes):
    chunks, tokens, _ = kv_chunks.shape
    rows = layer_input.shape[1]
    rows_out = rows // groups
    chips = groups // 2
    split = token_split(tokens, planes)
    lent = max(tokens - split, 128)
    jobs = (2 if split < tokens else 1) * chunks * planes
    segments = 3 if split < tokens else 2
    half, full = jnp.bfloat16, jnp.float32
    dma = pltpu.SemaphoreType.DMA
    vmem = pl.BlockSpec(memory_space=pltpu.VMEM)
    anywhere = pl.BlockSpec(memory_space=pl.ANY)
    return pl.pallas_call(
        functools.partial(sum_kernel, groups, planes, split, 1.0 / math.sqrt(tokens * groups)),
        out_shape=(
            jax.ShapeDtypeStruct((chunks, planes, rows_out, HD), full),
            jax.ShapeDtypeStruct((1, HD), full),
        ),
        in_specs=[anywhere, anywhere],
        out_specs=(vmem, vmem),
        scratch_shapes=[
            pltpu.VMEM((tokens, rows), half),
            pltpu.VMEM((rows, tokens), half),
            pltpu.VMEM((chunks, planes, tokens, HD), half),
            pltpu.VMEM((lent, rows), half),
            pltpu.VMEM((rows, lent), half),
            pltpu.VMEM((jobs, rows // 2, HD), full),
            pltpu.VMEM((jobs, rows // 2, HD), half),
            pltpu.VMEM((jobs, rows // 2, HD), half),
            pltpu.VMEM((jobs, chips - 1, rows_out, HD), half),
            pltpu.VMEM((jobs, chips - 1, rows_out, HD), half),
            pltpu.VMEM((chunks, planes, rows_out, HD), half),
            pltpu.VMEM((chunks, planes, rows_out, HD), half),
            pltpu.VMEM((chunks * planes, HD), full),
            pltpu.VMEM((groups * planes, 1, HD), full),
            dma,
            dma((chunks,)),
            dma((chunks, planes, segments)),
            dma((chunks, planes, segments)),
            dma((chunks, planes, segments)),
            dma,
            dma,
            dma((jobs,)),
            dma((jobs,)),
            dma((jobs, chips - 1)),
            dma((jobs, chips - 1)),
            dma((chunks, planes)),
            dma((chunks, planes)),
            dma,
            dma,
        ],
        compiler_params=pltpu.CompilerParams(
            collective_id=0, has_side_effects=True, vmem_limit_bytes=56 * 2**20
        ),
    )(kv_chunks, layer_input)


def per_device(
    layer_input, queries, keys_values, out_grads, log_sums, deltas, tile_fill, tile_cont, moment_first, moment_second
):
    groups, planes = lax.axis_size("dp"), lax.axis_size("tensor")
    keys, values = keys_values[:, 0], keys_values[:, 1]
    tokens = queries.shape[0]
    kv_local = keys.shape[1] // HD
    lse_rows = log_sums.astype(jnp.float32).T.reshape(kv_local, -1, tokens)
    delta_rows = deltas.astype(jnp.float32).T.reshape(kv_local, -1, tokens)
    kv_chunks = attend(queries, keys, values, out_grads, lse_rows, delta_rows, tile_fill, tile_cont)
    summed, square_row = sum_over_groups(kv_chunks, layer_input, groups, planes)
    rows_out = summed.shape[2]
    heads_kv = moment_second.shape[1]
    parts = summed.reshape(kv_local, 2, planes, rows_out, HD)
    proj_grads = parts.transpose(3, 1, 2, 0, 4).reshape(rows_out, 2, -1)
    squares = square_row[0, : 2 * heads_kv].reshape(kv_local, 2, planes).transpose(1, 2, 0).reshape(2, heads_kv)
    new_first = ADAM_ONE * moment_first + (1 - ADAM_ONE) * proj_grads
    new_second = ADAM_TWO * moment_second + (1 - ADAM_TWO) * squares / (D * HD)
    step_size = jnp.sqrt(new_second / (1 - ADAM_TWO**2)) + ADAM_EPS
    scaled = (new_first / (1 - ADAM_ONE**2)).reshape(rows_out, 2, heads_kv, -1)
    update = (scaled / step_size[None, :, :, None]).reshape(proj_grads.shape)
    return (update, new_first, new_second)


def solution(mesh):
    in_specs = (
        P("dp", "tensor"),
        P("dp", "tensor"),
        P("dp", None, "tensor"),
        P("dp", "tensor"),
        P("dp", "tensor"),
        P("dp", "tensor"),
        P(),
        P(),
        P(("tensor", "dp"), None, None),
        P(),
    )
    out_specs = (P(("tensor", "dp"), None, None), P(("tensor", "dp"), None, None), P())
    return jax.shard_map(
        per_device, mesh=mesh, in_specs=in_specs, out_specs=out_specs, check_vma=False
    )
```

```python
import functools
import math

import jax
import jax.numpy as jnp
from jax import lax
from jax.experimental import pallas as pl
from jax.experimental.pallas import tpu as pltpu
from jax.sharding import PartitionSpec as P

D = 4096
HD = 128
GRAIN = 16

ADAM_ONE = 0.9
ADAM_TWO = 0.95
ADAM_EPS = 1e-08
MESH = pl.DeviceIdType.MESH
NT = (((1,), (1,)), ((), ()))


def attend_tiles(tiles, group_size, fill_ref, cont_ref, q_ref, kv_ref, do_ref, lse_ref, delta_ref, key_out, value_out):
    group = lax.axis_index("dp")
    tokens, _, local = kv_ref.shape
    block = tokens // tiles
    scale_qk = HD ** (-0.5)
    wide = 2 * group_size * block
    key_place = lax.broadcasted_iota(jnp.int32, (block, wide), 0)
    column = lax.broadcasted_iota(jnp.int32, (block, wide), 1)
    query_place = column % block
    is_next = column >= group_size * block

    def one_tile(h, tile):
        after = jnp.minimum(tile + 1, tiles - 1)
        here = pl.ds(pl.multiple_of(tile * block, block), block)
        there = pl.ds(pl.multiple_of(after * block, block), block)
        fill_here = fill_ref[group, tile]
        fill_there = jnp.where(tile + 1 < tiles, fill_ref[group, after] * (cont_ref[group, after] == 1).astype(jnp.int32), 0)
        heads = [slice((h * group_size + j) * HD, (h * group_size + j + 1) * HD) for j in range(group_size)]
        q_cat = jnp.concatenate([q_ref[w, j] for w in (here, there) for j in heads], 0)
        do_cat = jnp.concatenate([do_ref[w, j] for w in (here, there) for j in heads], 0)
        lse = jnp.concatenate([lse_ref[h, j : j + 1, w] for w in (here, there) for j in range(group_size)], 1)
        delta = jnp.concatenate([delta_ref[h, j : j + 1, w] for w in (here, there) for j in range(group_size)], 1)
        pairs = kv_ref[here].reshape(block, 2 * local)
        keys, values = pairs[:, h * HD : (h + 1) * HD], pairs[:, local + h * HD : local + (h + 1) * HD]
        scores = lax.dot_general(keys, q_cat, NT, preferred_element_type=jnp.float32) * scale_qk
        limit = jnp.where(is_next, fill_there, fill_here)
        allowed = (query_place < limit) & (is_next | (query_place >= key_place))
        prob = jnp.where(allowed, jnp.exp(scores - lse), 0.0)
        dprob = lax.dot_general(values, do_cat, NT, preferred_element_type=jnp.float32)
        dscore = prob * (dprob - delta)
        value_grad = jnp.dot(prob.astype(jnp.bfloat16), do_cat, preferred_element_type=jnp.float32)
        key_grad = jnp.dot(dscore.astype(jnp.bfloat16), q_cat, preferred_element_type=jnp.float32) * scale_qk
        key_out(h, here, key_grad.astype(jnp.bfloat16))
        value_out(h, here, value_grad.astype(jnp.bfloat16))

    return one_tile


def token_split(tokens, planes):
    if planes < 4 or tokens < 1024:
        return tokens
    return tokens - tokens * 5 // 16 // 128 * 128


def capacities(tokens):
    if tokens < 1024:
        return [tokens]
    return [tokens * part // 16 // 128 * 128 for part in (12, 13, 14)] + [tokens]


def find_sources(tile_fill, positions):
    tiles = tile_fill.shape[1]
    live = (tile_fill + GRAIN - 1) // GRAIN
    upto = jnp.arange(tiles)[:, None] >= jnp.arange(tiles)[None, :]
    ends = jnp.sum(jnp.where(upto[None], live[:, None, :], 0), axis=2)
    group = jnp.arange(positions // GRAIN)
    passed = group[None, :, None] >= ends[:, None, :]
    skipped = positions // tiles // GRAIN - live
    source = group[None, :] + jnp.sum(jnp.where(passed, skipped[:, None, :], 0), axis=2)
    return jnp.minimum(source, positions // GRAIN), jnp.max(jnp.sum(live, axis=1)) * GRAIN


def sum_kernel(
    groups, planes, tiles, split, inv,
    fill_ref, cont_ref, source_ref, q_hbm, kv_hbm, do_hbm, lse_ref, delta_ref, layer_ref, out_ref, sq_ref,
    q_ref, kv_ref, do_ref, raw, packed, layer, flipped, gathered, lent, lent_flipped, keep, pair_send, pair_recv, chip_send, chip_recv,
    part_send, part_recv, squares, sq_all,
    load_sem, own_sem, kv_right, kv_left, kv_recv, lent_ssem, lent_rsem, pair_ssem, pair_rsem, chip_ssem, chip_rsem,
    part_ssem, part_rsem, sq_ssem, sq_rsem,
):
    me, plane = lax.axis_index("dp"), lax.axis_index("tensor")
    chips = groups // 2
    chip, core = me // 2, me % 2
    partner = me + 1 - 2 * core
    chunks, _, tokens, _ = gathered.shape
    positions = q_ref.shape[0]
    packing = tokens < positions
    rows = layer_ref.shape[-1]
    rows_out = rows // groups
    half = rows // 2
    events = planes * chunks
    lending = split < tokens
    is_end = (plane == 0) | (plane == planes - 1)
    is_helper = (plane == 1) | (plane == planes - 2)
    helped = jnp.where(plane == 1, 0, planes - 1)
    helper = jnp.where(plane == 0, 1, planes - 2)
    mid = split // 2 // (positions // tiles) * (positions // tiles)
    segments = ((split, tokens - split), (0, mid), (mid, split - mid)) if lending else ((0, mid), (mid, split - mid))

    loads = [
        pltpu.make_async_copy(source, target, own_sem.at[i])
        for i, (source, target) in enumerate(((kv_hbm, kv_ref), (q_hbm, q_ref), (do_hbm, do_ref)))
    ]
    for load in loads:
        load.start()
    rows_held = layer.at[pl.ds(0, positions // GRAIN)] if packing else layer
    layer_load = pltpu.make_async_copy(layer_ref, rows_held, load_sem)
    layer_load.start()

    barrier = pltpu.get_barrier_semaphore()
    mine = me * planes + plane

    def greet(step, carry):
        other = lax.rem(mine + step, groups * planes)
        pl.semaphore_signal(barrier, inc=1, device_id=(other // planes, other % planes), device_id_type=MESH)
        return carry

    lax.fori_loop(1, groups * planes, greet, 0)
    pl.semaphore_wait(barrier, groups * planes - 1)

    far = jnp.where(plane < planes // 2, 1, -1)
    near_count = jnp.minimum(plane, planes - 1 - plane)

    def piece_of(w):
        turn = (w + 1) // 2
        swing = jnp.where(w % 2 == 1, turn, -turn)
        return plane + far * jnp.where(w <= 2 * near_count, swing, w - near_count)

    def turn_of(e):
        k = e - 2 * chunks
        last, odd = k == 2 * chunks - 1, k % 2 == 1
        mixed = (planes >= 4) & (k >= 0) & (k < 2 * chunks)
        w = jnp.where(last | (jnp.logical_not(odd) & (k > 0)), 3, 2)
        c = jnp.where(last, chunks - 1, jnp.where(odd, (k + 1) // 2, jnp.maximum(k // 2 - 1, 0)))
        return jnp.where(mixed, w, e // chunks), jnp.where(mixed, c, e % chunks)

    def place(e):
        w, c = turn_of(e)
        return c, piece_of(w)

    def lend_copy():
        return pltpu.make_async_remote_copy(
            src_ref=(packed if packing else layer_ref).at[pl.ds(split, tokens - split), :], dst_ref=lent, send_sem=lent_ssem,
            recv_sem=lent_rsem, device_id=(me, helper), device_id_type=MESH,
        )

    def move(c, p, s, right):
        start, size = segments[s]
        where = gathered.at[c, p, pl.ds(start, size)]
        to = jnp.minimum(plane + 1, planes - 1) if right else jnp.maximum(plane - 1, 0)
        return pltpu.make_async_remote_copy(
            src_ref=where, dst_ref=where, send_sem=(kv_right if right else kv_left).at[c, p, s],
            recv_sem=kv_recv.at[c, p, s], device_id=(me, to), device_id_type=MESH,
        )

    def passes(p, s, right):
        lent_part = lending and s == 0
        if right:
            there = plane < planes - 2 if lent_part else plane < planes - 1
            return (p <= plane) & there
        there = plane > 1 if lent_part else plane > 0
        return (p >= plane) & there

    def pass_on(c, p, s):
        for right in (True, False):
            @pl.when(passes(p, s, right))
            def _():
                move(c, p, s, right).start()

    def arrive(c, p, s):
        if lending and s == 0:
            @pl.when(jnp.logical_not(is_end))
            def _():
                move(c, p, s, True).wait_recv()
        else:
            move(c, p, s, True).wait_recv()

    row_block = min(256, half)

    def multiply(source, lhs_from, rhs_from, length, c, p, job):
        weights = (c, p, pl.ds(rhs_from, length))

        def sent(i, carry):
            at = pl.multiple_of(i * row_block, row_block)
            pair_send[job, pl.ds(at, row_block), :] = jnp.dot(
                source[pl.ds(half + at, row_block), pl.ds(lhs_from, length)], gathered[weights],
                preferred_element_type=jnp.float32,
            ).astype(jnp.bfloat16)
            return carry

        def kept(i, carry):
            at = pl.multiple_of(i * row_block, row_block)
            keep[job, pl.ds(at, row_block), :] = jnp.dot(
                source[pl.ds(at, row_block), pl.ds(lhs_from, length)], gathered[weights],
                preferred_element_type=jnp.float32,
            )
            return carry

        lax.fori_loop(0, half // row_block, sent, 0)
        pair_copy(job).start()
        lax.fori_loop(0, half // row_block, kept, 0)

    def slice_of(k):
        return pl.ds(pl.multiple_of(k * rows_out, rows_out), rows_out)

    def pair_copy(job):
        return pltpu.make_async_remote_copy(
            src_ref=pair_send.at[job], dst_ref=pair_recv.at[job], send_sem=pair_ssem.at[job],
            recv_sem=pair_rsem.at[job], device_id=(partner, plane), device_id_type=MESH,
        )

    def chip_copy(job, step):
        other = lax.rem(chip + step, chips)
        return pltpu.make_async_remote_copy(
            src_ref=chip_send.at[job, step - 1], dst_ref=chip_recv.at[job, step - 1],
            send_sem=chip_ssem.at[job, step - 1], recv_sem=chip_rsem.at[job, step - 1],
            device_id=(2 * other + core, plane), device_id_type=MESH,
        )

    def part_copy(c, p):
        return pltpu.make_async_remote_copy(
            src_ref=part_send.at[c, p], dst_ref=part_recv.at[c, p], send_sem=part_ssem.at[c, p],
            recv_sem=part_rsem.at[c, p], device_id=(me, helped), device_id_type=MESH,
        )

    def own_job(c, p):
        return c * planes + p

    def part_job(c, p):
        return events + c * planes + p

    def scatter(job):
        pair_copy(job).wait_recv()
        for step in range(1, chips):
            other = slice_of(lax.rem(chip + step, chips))
            both = keep[job, other, :] + pair_recv[job, other, :].astype(jnp.float32)
            chip_send[job, step - 1] = both.astype(jnp.bfloat16)
            chip_copy(job, step).start()

    def total_of(job):
        mine = slice_of(chip)
        total = keep[job, mine, :] + pair_recv[job, mine, :].astype(jnp.float32)
        for step in range(1, chips):
            chip_copy(job, step).wait_recv()
            total = total + chip_recv[job, step - 1].astype(jnp.float32)
        return total

    def finish(c, p, total):
        total = total * inv
        out_ref[c, p] = total
        squares[pl.ds(c * planes + p, 1), :] = jnp.sum(total * total, axis=0, keepdims=True)

    def helped_total(c, p, total):
        part_copy(c, p).wait_recv()
        return total + part_recv[c, p].astype(jnp.float32)

    def gather_own(e):
        w, c = turn_of(e)
        p = piece_of(w)
        total = total_of(own_job(c, p))
        if not lending:
            finish(c, p, total)
            return
        plain = jnp.logical_not(is_end) | (w == 0)

        @pl.when(plain)
        def _():
            finish(c, p, total)

        @pl.when(is_end & (w >= 3))
        def _():
            finish(c, p, helped_total(c, p, total))

        @pl.when(is_end & ((w == 1) | (w == 2)))
        def _():
            out_ref[c, p] = total

    def late_finish(e):
        turn, c = turn_of(e)

        @pl.when(is_end & (turn == 3))
        def _():
            for w in (1, 2):
                p = piece_of(w)
                finish(c, p, helped_total(c, p, out_ref[c, p]))

    def for_parts(e, act):
        w, c = turn_of(e)

        @pl.when(is_helper & (w == 2))
        def _():
            def both(i, carry):
                act(c, piece_of(i))
                return carry

            lax.fori_loop(0, 2, both, 0)

        @pl.when(is_helper & (w >= 3))
        def _():
            act(c, piece_of(w))

    def part_multiply(c, p):
        multiply(lent_flipped, 0, split, tokens - split, c, p, part_job(c, p))

    def part_scatter(c, p):
        scatter(part_job(c, p))

    def part_gather(c, p):
        part_send[c, p] = total_of(part_job(c, p)).astype(jnp.bfloat16)
        part_copy(c, p).start()

    unit = min(128, rows_out)
    flip_block = 128

    def flip(source, target, i, carry):
        turned = source[:, pl.ds(pl.multiple_of(i * flip_block, flip_block), flip_block)].T
        for sub in range(flip_block // unit):
            start = i * flip_block + sub * unit
            piece = start // rows_out
            owner = piece // 2 + jnp.where(piece % 2 == core, 0, chips)
            to = pl.multiple_of(owner * rows_out + start % rows_out, unit)
            target[pl.ds(to, unit), :] = turned[sub * unit : (sub + 1) * unit]
        return carry

    block = positions // tiles
    def pack_layer(start, size):
        def one(g, carry):
            to = pl.multiple_of(g * GRAIN, GRAIN)
            packed[pl.ds(to, GRAIN), :] = layer[source_ref[me, g]]
            return carry

        lax.fori_loop(start // GRAIN, (start + size) // GRAIN, one, 0, unroll=4)

    def pack_own(h, start, size):
        def one(g, carry):
            to = pl.multiple_of(g * GRAIN, GRAIN)
            for c in (2 * h, 2 * h + 1):
                gathered[c, plane, pl.ds(to, GRAIN), :] = raw[c, source_ref[me, g]]
            return carry

        lax.fori_loop(start // GRAIN, (start + size) // GRAIN, one, 0, unroll=4)

    if packing:
        for c in range(chunks):
            raw[c, positions // GRAIN] = jnp.zeros((GRAIN, HD), jnp.bfloat16)
        layer[positions // GRAIN] = jnp.zeros(layer.shape[1:], jnp.bfloat16)
        layer_load.wait()
        pack_layer(split, tokens - split)
    if lending:
        @pl.when(is_end)
        def _():
            lend_copy().start()

    for load in loads:
        load.wait()

    def put(offset):
        def store(h, where, value):
            if packing:
                groups_of = pl.ds(where.start // GRAIN, where.size // GRAIN)
                raw[2 * h + offset, groups_of] = value.reshape(where.size // GRAIN, GRAIN, HD)
            else:
                gathered[2 * h + offset, plane, where, :] = value

        return store

    group_size = q_ref.shape[1] // (chunks // 2 * HD)
    one_tile = attend_tiles(
        tiles, group_size, fill_ref, cont_ref, q_ref, kv_ref, do_ref, lse_ref, delta_ref, put(0), put(1)
    )

    def attend(h, first, last):
        def tile_step(tile, carry):
            one_tile(h, tile)
            return carry

        lax.fori_loop(first, last, tile_step, 0)

    for h in range(chunks // 2):
        if packing:
            attend(h, 0, tiles)
        for s, (start, size) in enumerate(segments):
            if packing:
                pack_own(h, start, size)
            else:
                attend(h, start // block, (start + size) // block)
            for c in (2 * h, 2 * h + 1):
                pass_on(c, plane, s)

    if packing:
        pack_layer(0, split)
    else:
        layer_load.wait()
    lax.fori_loop(0, rows // flip_block, functools.partial(flip, packed if packing else layer, flipped), 0)

    def one_event(e, carry):
        w, c = turn_of(e)
        p = piece_of(w)

        @pl.when(w > 0)
        def _():
            for s in range(len(segments)):
                arrive(c, p, s)
                pass_on(c, p, s)

        if lending:
            @pl.when(is_helper & (e == 2 * chunks))
            def _():
                lend_copy().wait_recv()
                lax.fori_loop(0, rows // flip_block, functools.partial(flip, lent, lent_flipped), 0)

            for_parts(e, part_multiply)
            short = is_end & (w > 0)

            @pl.when(short)
            def _():
                multiply(flipped, 0, 0, split, c, p, own_job(c, p))

            @pl.when(jnp.logical_not(short))
            def _():
                multiply(flipped, 0, 0, tokens, c, p, own_job(c, p))
        else:
            multiply(flipped, 0, 0, tokens, c, p, own_job(c, p))

        @pl.when(e >= 1)
        def _():
            if lending:
                for_parts(e - 1, part_scatter)
            scatter(own_job(*place(e - 1)))

        @pl.when(e >= 2)
        def _():
            if lending:
                for_parts(e - 2, part_gather)
            gather_own(e - 2)

        if lending:
            late_finish(e)
        return carry

    lax.fori_loop(0, events, one_event, 0)
    if lending:
        for_parts(events - 1, part_scatter)
    scatter(own_job(*place(events - 1)))
    if lending:
        for_parts(events - 2, part_gather)
        for_parts(events - 1, part_gather)
    gather_own(events - 2)
    gather_own(events - 1)

    lane_sums = jnp.sum(squares[...], axis=1, keepdims=True)
    row = lax.broadcasted_iota(jnp.int32, (squares.shape[0], HD), 0)
    lane = lax.broadcasted_iota(jnp.int32, (squares.shape[0], HD), 1)
    sq_all[mine] = jnp.sum(jnp.where(row == lane, lane_sums, 0.0), axis=0, keepdims=True)

    def sq_copy(step):
        other = lax.rem(mine + step, groups * planes)
        return pltpu.make_async_remote_copy(
            src_ref=sq_all.at[mine], dst_ref=sq_all.at[mine], send_sem=sq_ssem, recv_sem=sq_rsem,
            device_id=(other // planes, other % planes), device_id_type=MESH,
        )

    def send_squares(step, carry):
        sq_copy(step).start()
        return carry

    lax.fori_loop(1, groups * planes, send_squares, 0)
    others = sq_all.at[pl.ds(0, groups * planes - 1)]
    pltpu.make_async_copy(others, others, sq_rsem).wait()
    sq_ref[...] = jnp.sum(sq_all[...], axis=0)
    pltpu.make_async_copy(others, others, sq_ssem).wait()

    if lending:
        @pl.when(is_end)
        def _():
            lend_copy().wait_send()

    def drain_job(job):
        pair_copy(job).wait_send()
        for step in range(1, chips):
            chip_copy(job, step).wait_send()

    def drain(e, carry):
        c, p = e // planes, e % planes
        drain_job(own_job(c, p))
        if lending:
            @pl.when(is_helper & (p != helped))
            def _():
                drain_job(part_job(c, p))
                part_copy(c, p).wait_send()

        for s in range(len(segments)):
            for right in (True, False):
                @pl.when(passes(p, s, right))
                def _():
                    move(c, p, s, right).wait_send()
        return carry

    lax.fori_loop(0, events, drain, 0)


def sum_over_groups(
    tile_fill, tile_cont, sources, queries, keys_values, out_grads, lse_rows, delta_rows, layer_input, groups, planes, number, tokens
):
    positions, _, local = keys_values.shape
    chunks = 2 * (local // HD)
    tiles = tile_fill.shape[1]
    rows = layer_input.shape[1]
    if tokens < positions:
        layer_input = layer_input.reshape(positions // GRAIN, GRAIN, rows)
    rows_out = rows // groups
    chips = groups // 2
    packing = tokens < positions
    split = token_split(tokens, planes)
    lent = max(tokens - split, 128)
    jobs = (2 if split < tokens else 1) * chunks * planes
    segments = 3 if split < tokens else 2
    half, full = jnp.bfloat16, jnp.float32
    dma = pltpu.SemaphoreType.DMA
    vmem = pl.BlockSpec(memory_space=pltpu.VMEM)
    anywhere = pl.BlockSpec(memory_space=pl.ANY)
    smem = pl.BlockSpec(memory_space=pltpu.SMEM)
    return pl.pallas_call(
        functools.partial(sum_kernel, groups, planes, tiles, split, 1.0 / math.sqrt(positions * groups)),
        out_shape=(
            jax.ShapeDtypeStruct((chunks, planes, rows_out, HD), full),
            jax.ShapeDtypeStruct((1, HD), full),
        ),
        in_specs=[smem, smem, smem, anywhere, anywhere, anywhere, vmem, vmem, anywhere],
        out_specs=(vmem, vmem),
        scratch_shapes=[
            pltpu.VMEM(queries.shape, half),
            pltpu.VMEM(keys_values.shape, half),
            pltpu.VMEM(out_grads.shape, half),
            pltpu.VMEM((chunks, positions // GRAIN + 1, GRAIN, HD) if packing else (GRAIN, HD), half),
            pltpu.VMEM((tokens, rows) if packing else (GRAIN, HD), half),
            pltpu.VMEM((positions // GRAIN + 1, GRAIN, rows) if packing else (positions, rows), half),
            pltpu.VMEM((rows, tokens), half),
            pltpu.VMEM((chunks, planes, tokens, HD), half),
            pltpu.VMEM((lent, rows), half),
            pltpu.VMEM((rows, lent), half),
            pltpu.VMEM((jobs, rows // 2, HD), full),
            pltpu.VMEM((jobs, rows // 2, HD), half),
            pltpu.VMEM((jobs, rows // 2, HD), half),
            pltpu.VMEM((jobs, chips - 1, rows_out, HD), half),
            pltpu.VMEM((jobs, chips - 1, rows_out, HD), half),
            pltpu.VMEM((chunks, planes, rows_out, HD), half),
            pltpu.VMEM((chunks, planes, rows_out, HD), half),
            pltpu.VMEM((chunks * planes, HD), full),
            pltpu.VMEM((groups * planes, 1, HD), full),
            dma,
            dma((3,)),
            dma((chunks, planes, segments)),
            dma((chunks, planes, segments)),
            dma((chunks, planes, segments)),
            dma,
            dma,
            dma((jobs,)),
            dma((jobs,)),
            dma((jobs, chips - 1)),
            dma((jobs, chips - 1)),
            dma((chunks, planes)),
            dma((chunks, planes)),
            dma,
            dma,
        ],
        compiler_params=pltpu.CompilerParams(
            collective_id=number, has_side_effects=True, vmem_limit_bytes=60 * 2**20
        ),
    )(tile_fill, tile_cont, sources, queries, keys_values, out_grads, lse_rows, delta_rows, layer_input)


def per_device(
    layer_input, queries, keys_values, out_grads, log_sums, deltas, tile_fill, tile_cont, moment_first, moment_second
):
    groups, planes = lax.axis_size("dp"), lax.axis_size("tensor")
    tokens = queries.shape[0]
    kv_local = keys_values.shape[2] // HD
    lse_rows = log_sums.astype(jnp.float32).T.reshape(kv_local, -1, tokens)
    delta_rows = deltas.astype(jnp.float32).T.reshape(kv_local, -1, tokens)
    lengths = capacities(tokens)
    sources, needed = find_sources(tile_fill, tokens)
    summed, square_row = lax.switch(
        sum((needed > length).astype(jnp.int32) for length in lengths[:-1]) if len(lengths) > 1 else 0,
        [
            functools.partial(sum_over_groups, groups=groups, planes=planes, number=i, tokens=length)
            for i, length in enumerate(lengths)
        ],
        tile_fill, tile_cont, sources, queries, keys_values, out_grads, lse_rows, delta_rows, layer_input,
    )
    rows_out = summed.shape[2]
    heads_kv = moment_second.shape[1]
    parts = summed.reshape(kv_local, 2, planes, rows_out, HD)
    proj_grads = parts.transpose(3, 1, 2, 0, 4).reshape(rows_out, 2, -1)
    squares = square_row[0, : 2 * heads_kv].reshape(kv_local, 2, planes).transpose(1, 2, 0).reshape(2, heads_kv)
    new_first = ADAM_ONE * moment_first + (1 - ADAM_ONE) * proj_grads
    new_second = ADAM_TWO * moment_second + (1 - ADAM_TWO) * squares / (D * HD)
    step_size = jnp.sqrt(new_second / (1 - ADAM_TWO**2)) + ADAM_EPS
    scaled = (new_first / (1 - ADAM_ONE**2)).reshape(rows_out, 2, heads_kv, -1)
    update = (scaled / step_size[None, :, :, None]).reshape(proj_grads.shape)
    return (update, new_first, new_second)


def solution(mesh):
    in_specs = (
        P("dp", "tensor"),
        P("dp", "tensor"),
        P("dp", None, "tensor"),
        P("dp", "tensor"),
        P("dp", "tensor"),
        P("dp", "tensor"),
        P(),
        P(),
        P(("tensor", "dp"), None, None),
        P(),
    )
    out_specs = (P(("tensor", "dp"), None, None), P(("tensor", "dp"), None, None), P())
    return jax.shard_map(
        per_device, mesh=mesh, in_specs=in_specs, out_specs=out_specs, check_vma=False
    )
```

```python
import functools
import math

import jax
import jax.numpy as jnp
from jax import lax
from jax.experimental import pallas as pl
from jax.experimental.pallas import tpu as pltpu
from jax.sharding import PartitionSpec as P

D = 4096
HD = 128
GRAIN = 16

ADAM_ONE = 0.9
ADAM_TWO = 0.95
ADAM_EPS = 1e-08
MESH = pl.DeviceIdType.MESH
NT = (((1,), (1,)), ((), ()))


def attend_tiles(tiles, group_size, fill_ref, cont_ref, q_ref, kv_ref, do_ref, lse_ref, delta_ref, key_out, value_out):
    group = lax.axis_index("dp")
    tokens, _, local = kv_ref.shape
    block = tokens // tiles
    scale_qk = HD ** (-0.5)
    wide = 2 * group_size * block
    key_place = lax.broadcasted_iota(jnp.int32, (block, wide), 0)
    column = lax.broadcasted_iota(jnp.int32, (block, wide), 1)
    query_place = column % block
    is_next = column >= group_size * block

    def one_tile(h, tile):
        after = jnp.minimum(tile + 1, tiles - 1)
        here = pl.ds(pl.multiple_of(tile * block, block), block)
        there = pl.ds(pl.multiple_of(after * block, block), block)
        fill_here = fill_ref[group, tile]
        fill_there = jnp.where(tile + 1 < tiles, fill_ref[group, after] * (cont_ref[group, after] == 1).astype(jnp.int32), 0)
        heads = [slice((h * group_size + j) * HD, (h * group_size + j + 1) * HD) for j in range(group_size)]
        q_cat = jnp.concatenate([q_ref[w, j] for w in (here, there) for j in heads], 0)
        do_cat = jnp.concatenate([do_ref[w, j] for w in (here, there) for j in heads], 0)
        lse = jnp.concatenate([lse_ref[h * group_size + j : h * group_size + j + 1, w] for w in (here, there) for j in range(group_size)], 1)
        delta = jnp.concatenate([delta_ref[h * group_size + j : h * group_size + j + 1, w] for w in (here, there) for j in range(group_size)], 1)
        pairs = kv_ref[here].reshape(block, 2 * local)
        keys, values = pairs[:, h * HD : (h + 1) * HD], pairs[:, local + h * HD : local + (h + 1) * HD]
        scores = lax.dot_general(keys, q_cat, NT, preferred_element_type=jnp.float32) * scale_qk
        limit = jnp.where(is_next, fill_there, fill_here)
        allowed = (query_place < limit) & (is_next | (query_place >= key_place))
        prob = jnp.where(allowed, jnp.exp(scores - lse), 0.0)
        dprob = lax.dot_general(values, do_cat, NT, preferred_element_type=jnp.float32)
        dscore = prob * (dprob - delta)
        value_grad = jnp.dot(prob.astype(jnp.bfloat16), do_cat, preferred_element_type=jnp.float32)
        key_grad = jnp.dot(dscore.astype(jnp.bfloat16), q_cat, preferred_element_type=jnp.float32) * scale_qk
        key_out(h, here, key_grad.astype(jnp.bfloat16))
        value_out(h, here, value_grad.astype(jnp.bfloat16))

    return one_tile


def token_split(tokens, planes):
    if planes < 4 or tokens < 1024:
        return tokens
    return tokens - tokens * 5 // 16 // 128 * 128


def capacities(tokens):
    if tokens < 1024:
        return [tokens]
    return [tokens * part // 16 // 128 * 128 for part in (12, 13, 14)] + [tokens]


def find_sources(tile_fill, positions):
    tiles = tile_fill.shape[1]
    live = (tile_fill + GRAIN - 1) // GRAIN
    upto = jnp.arange(tiles)[:, None] >= jnp.arange(tiles)[None, :]
    ends = jnp.sum(jnp.where(upto[None], live[:, None, :], 0), axis=2)
    group = jnp.arange(positions // GRAIN)
    passed = group[None, :, None] >= ends[:, None, :]
    skipped = positions // tiles // GRAIN - live
    source = group[None, :] + jnp.sum(jnp.where(passed, skipped[:, None, :], 0), axis=2)
    return jnp.minimum(source, positions // GRAIN), jnp.max(jnp.sum(live, axis=1)) * GRAIN


def sum_kernel(
    groups, planes, tiles, split, inv,
    fill_ref, cont_ref, source_ref, q_hbm, kv_hbm, do_hbm, lse_half, delta_half, layer_ref, out_ref, sq_ref,
    q_ref, kv_ref, do_ref, lse_ref, delta_ref, raw, packed, layer, flipped, gathered, lent, lent_flipped, keep, pair_send, pair_recv, chip_send, chip_recv,
    part_send, part_recv, squares, sq_all,
    load_sem, own_sem, kv_right, kv_left, kv_recv, lent_ssem, lent_rsem, pair_ssem, pair_rsem, chip_ssem, chip_rsem,
    part_ssem, part_rsem, sq_ssem, sq_rsem,
):
    me, plane = lax.axis_index("dp"), lax.axis_index("tensor")
    chips = groups // 2
    chip, core = me // 2, me % 2
    partner = me + 1 - 2 * core
    chunks, _, tokens, _ = gathered.shape
    positions = q_ref.shape[0]
    packing = tokens < positions
    rows = layer_ref.shape[-1]
    rows_out = rows // groups
    half = rows // 2
    events = planes * chunks
    lending = split < tokens
    is_end = (plane == 0) | (plane == planes - 1)
    is_helper = (plane == 1) | (plane == planes - 2)
    helped = jnp.where(plane == 1, 0, planes - 1)
    helper = jnp.where(plane == 0, 1, planes - 2)
    mid = split // 2 // (positions // tiles) * (positions // tiles)
    segments = ((split, tokens - split), (0, mid), (mid, split - mid)) if lending else ((0, mid), (mid, split - mid))

    loads = [
        pltpu.make_async_copy(source, target, own_sem.at[i])
        for i, (source, target) in enumerate(((kv_hbm, kv_ref), (q_hbm, q_ref), (do_hbm, do_ref)))
    ]
    for load in loads:
        load.start()
    rows_held = layer.at[pl.ds(0, positions // GRAIN)] if packing else layer
    layer_load = pltpu.make_async_copy(layer_ref, rows_held, load_sem)
    layer_load.start()

    barrier = pltpu.get_barrier_semaphore()
    mine = me * planes + plane

    def greet(step, carry):
        other = lax.rem(mine + step, groups * planes)
        pl.semaphore_signal(barrier, inc=1, device_id=(other // planes, other % planes), device_id_type=MESH)
        return carry

    lax.fori_loop(1, groups * planes, greet, 0)
    pl.semaphore_wait(barrier, groups * planes - 1)

    far = jnp.where(plane < planes // 2, 1, -1)
    near_count = jnp.minimum(plane, planes - 1 - plane)

    def piece_of(w):
        turn = (w + 1) // 2
        swing = jnp.where(w % 2 == 1, turn, -turn)
        return plane + far * jnp.where(w <= 2 * near_count, swing, w - near_count)

    def turn_of(e):
        k = e - 2 * chunks
        last, odd = k == 2 * chunks - 1, k % 2 == 1
        mixed = (planes >= 4) & (k >= 0) & (k < 2 * chunks)
        w = jnp.where(last | (jnp.logical_not(odd) & (k > 0)), 3, 2)
        c = jnp.where(last, chunks - 1, jnp.where(odd, (k + 1) // 2, jnp.maximum(k // 2 - 1, 0)))
        return jnp.where(mixed, w, e // chunks), jnp.where(mixed, c, e % chunks)

    def place(e):
        w, c = turn_of(e)
        return c, piece_of(w)

    def lend_copy():
        return pltpu.make_async_remote_copy(
            src_ref=(packed if packing else layer_ref).at[pl.ds(split, tokens - split), :], dst_ref=lent, send_sem=lent_ssem,
            recv_sem=lent_rsem, device_id=(me, helper), device_id_type=MESH,
        )

    def move(c, p, s, right):
        start, size = segments[s]
        where = gathered.at[c, p, pl.ds(start, size)]
        to = jnp.minimum(plane + 1, planes - 1) if right else jnp.maximum(plane - 1, 0)
        return pltpu.make_async_remote_copy(
            src_ref=where, dst_ref=where, send_sem=(kv_right if right else kv_left).at[c, p, s],
            recv_sem=kv_recv.at[c, p, s], device_id=(me, to), device_id_type=MESH,
        )

    def passes(p, s, right):
        lent_part = lending and s == 0
        if right:
            there = plane < planes - 2 if lent_part else plane < planes - 1
            return (p <= plane) & there
        there = plane > 1 if lent_part else plane > 0
        return (p >= plane) & there

    def pass_on(c, p, s):
        for right in (True, False):
            @pl.when(passes(p, s, right))
            def _():
                move(c, p, s, right).start()

    def arrive(c, p, s):
        if lending and s == 0:
            @pl.when(jnp.logical_not(is_end))
            def _():
                move(c, p, s, True).wait_recv()
        else:
            move(c, p, s, True).wait_recv()

    row_block = min(256, half)

    def multiply(source, lhs_from, rhs_from, length, c, p, job):
        weights = (c, p, pl.ds(rhs_from, length))

        def sent(i, carry):
            at = pl.multiple_of(i * row_block, row_block)
            pair_send[job, pl.ds(at, row_block), :] = jnp.dot(
                source[pl.ds(half + at, row_block), pl.ds(lhs_from, length)], gathered[weights],
                preferred_element_type=jnp.float32,
            ).astype(jnp.bfloat16)
            return carry

        def kept(i, carry):
            at = pl.multiple_of(i * row_block, row_block)
            keep[job, pl.ds(at, row_block), :] = jnp.dot(
                source[pl.ds(at, row_block), pl.ds(lhs_from, length)], gathered[weights],
                preferred_element_type=jnp.float32,
            )
            return carry

        lax.fori_loop(0, half // row_block, sent, 0)
        pair_copy(job).start()
        lax.fori_loop(0, half // row_block, kept, 0)

    def slice_of(k):
        return pl.ds(pl.multiple_of(k * rows_out, rows_out), rows_out)

    def pair_copy(job):
        return pltpu.make_async_remote_copy(
            src_ref=pair_send.at[job], dst_ref=pair_recv.at[job], send_sem=pair_ssem.at[job],
            recv_sem=pair_rsem.at[job], device_id=(partner, plane), device_id_type=MESH,
        )

    def chip_copy(job, step):
        other = lax.rem(chip + step, chips)
        return pltpu.make_async_remote_copy(
            src_ref=chip_send.at[job, step - 1], dst_ref=chip_recv.at[job, step - 1],
            send_sem=chip_ssem.at[job, step - 1], recv_sem=chip_rsem.at[job, step - 1],
            device_id=(2 * other + core, plane), device_id_type=MESH,
        )

    def part_copy(c, p):
        return pltpu.make_async_remote_copy(
            src_ref=part_send.at[c, p], dst_ref=part_recv.at[c, p], send_sem=part_ssem.at[c, p],
            recv_sem=part_rsem.at[c, p], device_id=(me, helped), device_id_type=MESH,
        )

    def own_job(c, p):
        return c * planes + p

    def part_job(c, p):
        return events + c * planes + p

    def scatter(job):
        pair_copy(job).wait_recv()
        for step in range(1, chips):
            other = slice_of(lax.rem(chip + step, chips))
            both = keep[job, other, :] + pair_recv[job, other, :].astype(jnp.float32)
            chip_send[job, step - 1] = both.astype(jnp.bfloat16)
            chip_copy(job, step).start()

    def total_of(job):
        mine = slice_of(chip)
        total = keep[job, mine, :] + pair_recv[job, mine, :].astype(jnp.float32)
        for step in range(1, chips):
            chip_copy(job, step).wait_recv()
            total = total + chip_recv[job, step - 1].astype(jnp.float32)
        return total

    def finish(c, p, total):
        total = total * inv
        out_ref[c, p] = total
        squares[pl.ds(c * planes + p, 1), :] = jnp.sum(total * total, axis=0, keepdims=True)

    def helped_total(c, p, total):
        part_copy(c, p).wait_recv()
        return total + part_recv[c, p].astype(jnp.float32)

    def gather_own(e):
        w, c = turn_of(e)
        p = piece_of(w)
        total = total_of(own_job(c, p))
        if not lending:
            finish(c, p, total)
            return
        plain = jnp.logical_not(is_end) | (w == 0)

        @pl.when(plain)
        def _():
            finish(c, p, total)

        @pl.when(is_end & (w >= 3))
        def _():
            finish(c, p, helped_total(c, p, total))

        @pl.when(is_end & ((w == 1) | (w == 2)))
        def _():
            out_ref[c, p] = total

    def late_finish(e):
        turn, c = turn_of(e)

        @pl.when(is_end & (turn == 3))
        def _():
            for w in (1, 2):
                p = piece_of(w)
                finish(c, p, helped_total(c, p, out_ref[c, p]))

    def for_parts(e, act):
        w, c = turn_of(e)

        @pl.when(is_helper & (w == 2))
        def _():
            def both(i, carry):
                act(c, piece_of(i))
                return carry

            lax.fori_loop(0, 2, both, 0)

        @pl.when(is_helper & (w >= 3))
        def _():
            act(c, piece_of(w))

    def part_multiply(c, p):
        multiply(lent_flipped, 0, split, tokens - split, c, p, part_job(c, p))

    def part_scatter(c, p):
        scatter(part_job(c, p))

    def part_gather(c, p):
        part_send[c, p] = total_of(part_job(c, p)).astype(jnp.bfloat16)
        part_copy(c, p).start()

    unit = min(128, rows_out)
    flip_block = 128

    def flip(source, target, i, carry):
        turned = source[:, pl.ds(pl.multiple_of(i * flip_block, flip_block), flip_block)].T
        for sub in range(flip_block // unit):
            start = i * flip_block + sub * unit
            piece = start // rows_out
            owner = piece // 2 + jnp.where(piece % 2 == core, 0, chips)
            to = pl.multiple_of(owner * rows_out + start % rows_out, unit)
            target[pl.ds(to, unit), :] = turned[sub * unit : (sub + 1) * unit]
        return carry

    block = positions // tiles
    def pack_layer(start, size):
        def one(g, carry):
            to = pl.multiple_of(g * GRAIN, GRAIN)
            packed[pl.ds(to, GRAIN), :] = layer[source_ref[me, g]]
            return carry

        lax.fori_loop(start // GRAIN, (start + size) // GRAIN, one, 0, unroll=4)

    def pack_own(h, start, size):
        def one(g, carry):
            to = pl.multiple_of(g * GRAIN, GRAIN)
            for c in (2 * h, 2 * h + 1):
                gathered[c, plane, pl.ds(to, GRAIN), :] = raw[c, source_ref[me, g]]
            return carry

        lax.fori_loop(start // GRAIN, (start + size) // GRAIN, one, 0, unroll=4)

    if packing:
        for c in range(chunks):
            raw[c, positions // GRAIN] = jnp.zeros((GRAIN, HD), jnp.bfloat16)
        layer[positions // GRAIN] = jnp.zeros(layer.shape[1:], jnp.bfloat16)
        layer_load.wait()
        pack_layer(split, tokens - split)
    if lending:
        @pl.when(is_end)
        def _():
            lend_copy().start()

    lse_ref[...] = lse_half[...].astype(jnp.float32)
    delta_ref[...] = delta_half[...].astype(jnp.float32)
    for load in loads:
        load.wait()

    def put(offset):
        def store(h, where, value):
            if packing:
                groups_of = pl.ds(where.start // GRAIN, where.size // GRAIN)
                raw[2 * h + offset, groups_of] = value.reshape(where.size // GRAIN, GRAIN, HD)
            else:
                gathered[2 * h + offset, plane, where, :] = value

        return store

    group_size = q_ref.shape[1] // (chunks // 2 * HD)
    one_tile = attend_tiles(
        tiles, group_size, fill_ref, cont_ref, q_ref, kv_ref, do_ref, lse_ref, delta_ref, put(0), put(1)
    )

    def attend(h, first, last):
        def tile_step(tile, carry):
            one_tile(h, tile)
            return carry

        lax.fori_loop(first, last, tile_step, 0, unroll=2 if packing else 1)

    for h in range(chunks // 2):
        if packing:
            attend(h, 0, tiles)
        for s, (start, size) in enumerate(segments):
            if packing:
                pack_own(h, start, size)
            else:
                attend(h, start // block, (start + size) // block)
            for c in (2 * h, 2 * h + 1):
                pass_on(c, plane, s)

    if packing:
        pack_layer(0, split)
    else:
        layer_load.wait()
    lax.fori_loop(0, rows // flip_block, functools.partial(flip, packed if packing else layer, flipped), 0)

    def one_event(e, carry):
        w, c = turn_of(e)
        p = piece_of(w)

        @pl.when(w > 0)
        def _():
            for s in range(len(segments)):
                arrive(c, p, s)
                pass_on(c, p, s)

        if lending:
            @pl.when(is_helper & (e == 2 * chunks))
            def _():
                lend_copy().wait_recv()
                lax.fori_loop(0, rows // flip_block, functools.partial(flip, lent, lent_flipped), 0)

            for_parts(e, part_multiply)
            short = is_end & (w > 0)

            @pl.when(short)
            def _():
                multiply(flipped, 0, 0, split, c, p, own_job(c, p))

            @pl.when(jnp.logical_not(short))
            def _():
                multiply(flipped, 0, 0, tokens, c, p, own_job(c, p))
        else:
            multiply(flipped, 0, 0, tokens, c, p, own_job(c, p))

        @pl.when(e >= 1)
        def _():
            if lending:
                for_parts(e - 1, part_scatter)
            scatter(own_job(*place(e - 1)))

        @pl.when(e >= 2)
        def _():
            if lending:
                for_parts(e - 2, part_gather)
            gather_own(e - 2)

        if lending:
            late_finish(e)
        return carry

    lax.fori_loop(0, events, one_event, 0)
    if lending:
        for_parts(events - 1, part_scatter)
    scatter(own_job(*place(events - 1)))
    if lending:
        for_parts(events - 2, part_gather)
        for_parts(events - 1, part_gather)
    gather_own(events - 2)
    gather_own(events - 1)

    lane_sums = jnp.sum(squares[...], axis=1, keepdims=True)
    row = lax.broadcasted_iota(jnp.int32, (squares.shape[0], HD), 0)
    lane = lax.broadcasted_iota(jnp.int32, (squares.shape[0], HD), 1)
    sq_all[mine] = jnp.sum(jnp.where(row == lane, lane_sums, 0.0), axis=0, keepdims=True)

    def sq_copy(step):
        other = lax.rem(mine + step, groups * planes)
        return pltpu.make_async_remote_copy(
            src_ref=sq_all.at[mine], dst_ref=sq_all.at[mine], send_sem=sq_ssem, recv_sem=sq_rsem,
            device_id=(other // planes, other % planes), device_id_type=MESH,
        )

    def send_squares(step, carry):
        sq_copy(step).start()
        return carry

    lax.fori_loop(1, groups * planes, send_squares, 0)
    others = sq_all.at[pl.ds(0, groups * planes - 1)]
    pltpu.make_async_copy(others, others, sq_rsem).wait()
    sq_ref[...] = jnp.sum(sq_all[...], axis=0)
    pltpu.make_async_copy(others, others, sq_ssem).wait()

    if lending:
        @pl.when(is_end)
        def _():
            lend_copy().wait_send()

    def drain_job(job):
        pair_copy(job).wait_send()
        for step in range(1, chips):
            chip_copy(job, step).wait_send()

    def drain(e, carry):
        c, p = e // planes, e % planes
        drain_job(own_job(c, p))
        if lending:
            @pl.when(is_helper & (p != helped))
            def _():
                drain_job(part_job(c, p))
                part_copy(c, p).wait_send()

        for s in range(len(segments)):
            for right in (True, False):
                @pl.when(passes(p, s, right))
                def _():
                    move(c, p, s, right).wait_send()
        return carry

    lax.fori_loop(0, events, drain, 0)


def sum_over_groups(
    tile_fill, tile_cont, sources, queries, keys_values, out_grads, lse_rows, delta_rows, layer_input, groups, planes, number, tokens
):
    positions, _, local = keys_values.shape
    chunks = 2 * (local // HD)
    tiles = tile_fill.shape[1]
    rows = layer_input.shape[1]
    if tokens < positions:
        layer_input = layer_input.reshape(positions // GRAIN, GRAIN, rows)
    rows_out = rows // groups
    chips = groups // 2
    packing = tokens < positions
    split = token_split(tokens, planes)
    lent = max(tokens - split, 128)
    jobs = (2 if split < tokens else 1) * chunks * planes
    segments = 3 if split < tokens else 2
    half, full = jnp.bfloat16, jnp.float32
    dma = pltpu.SemaphoreType.DMA
    vmem = pl.BlockSpec(memory_space=pltpu.VMEM)
    anywhere = pl.BlockSpec(memory_space=pl.ANY)
    smem = pl.BlockSpec(memory_space=pltpu.SMEM)
    return pl.pallas_call(
        functools.partial(sum_kernel, groups, planes, tiles, split, 1.0 / math.sqrt(positions * groups)),
        out_shape=(
            jax.ShapeDtypeStruct((chunks, planes, rows_out, HD), full),
            jax.ShapeDtypeStruct((1, HD), full),
        ),
        in_specs=[smem, smem, smem, anywhere, anywhere, anywhere, vmem, vmem, anywhere],
        out_specs=(vmem, vmem),
        scratch_shapes=[
            pltpu.VMEM(queries.shape, half),
            pltpu.VMEM(keys_values.shape, half),
            pltpu.VMEM(out_grads.shape, half),
            pltpu.VMEM(lse_rows.shape, full),
            pltpu.VMEM(delta_rows.shape, full),
            pltpu.VMEM((chunks, positions // GRAIN + 1, GRAIN, HD) if packing else (GRAIN, HD), half),
            pltpu.VMEM((tokens, rows) if packing else (GRAIN, HD), half),
            pltpu.VMEM((positions // GRAIN + 1, GRAIN, rows) if packing else (positions, rows), half),
            pltpu.VMEM((rows, tokens), half),
            pltpu.VMEM((chunks, planes, tokens, HD), half),
            pltpu.VMEM((lent, rows), half),
            pltpu.VMEM((rows, lent), half),
            pltpu.VMEM((jobs, rows // 2, HD), full),
            pltpu.VMEM((jobs, rows // 2, HD), half),
            pltpu.VMEM((jobs, rows // 2, HD), half),
            pltpu.VMEM((jobs, chips - 1, rows_out, HD), half),
            pltpu.VMEM((jobs, chips - 1, rows_out, HD), half),
            pltpu.VMEM((chunks, planes, rows_out, HD), half),
            pltpu.VMEM((chunks, planes, rows_out, HD), half),
            pltpu.VMEM((chunks * planes, HD), full),
            pltpu.VMEM((groups * planes, 1, HD), full),
            dma,
            dma((3,)),
            dma((chunks, planes, segments)),
            dma((chunks, planes, segments)),
            dma((chunks, planes, segments)),
            dma,
            dma,
            dma((jobs,)),
            dma((jobs,)),
            dma((jobs, chips - 1)),
            dma((jobs, chips - 1)),
            dma((chunks, planes)),
            dma((chunks, planes)),
            dma,
            dma,
        ],
        compiler_params=pltpu.CompilerParams(
            collective_id=number, has_side_effects=True, vmem_limit_bytes=60 * 2**20
        ),
    )(tile_fill, tile_cont, sources, queries, keys_values, out_grads, lse_rows, delta_rows, layer_input)


def per_device(
    layer_input, queries, keys_values, out_grads, log_sums, deltas, tile_fill, tile_cont, moment_first, moment_second
):
    groups, planes = lax.axis_size("dp"), lax.axis_size("tensor")
    tokens = queries.shape[0]
    kv_local = keys_values.shape[2] // HD
    lse_rows, delta_rows = log_sums.T, deltas.T
    lengths = capacities(tokens)
    sources, needed = find_sources(tile_fill, tokens)
    summed, square_row = lax.switch(
        sum((needed > length).astype(jnp.int32) for length in lengths[:-1]) if len(lengths) > 1 else 0,
        [
            functools.partial(sum_over_groups, groups=groups, planes=planes, number=i, tokens=length)
            for i, length in enumerate(lengths)
        ],
        tile_fill, tile_cont, sources, queries, keys_values, out_grads, lse_rows, delta_rows, layer_input,
    )
    rows_out = summed.shape[2]
    heads_kv = moment_second.shape[1]
    parts = summed.reshape(kv_local, 2, planes, rows_out, HD)
    proj_grads = parts.transpose(3, 1, 2, 0, 4).reshape(rows_out, 2, -1)
    squares = square_row[0, : 2 * heads_kv].reshape(kv_local, 2, planes).transpose(1, 2, 0).reshape(2, heads_kv)
    new_first = ADAM_ONE * moment_first + (1 - ADAM_ONE) * proj_grads
    new_second = ADAM_TWO * moment_second + (1 - ADAM_TWO) * squares / (D * HD)
    step_size = jnp.sqrt(new_second / (1 - ADAM_TWO**2)) + ADAM_EPS
    scaled = (new_first / (1 - ADAM_ONE**2)).reshape(rows_out, 2, heads_kv, -1)
    update = (scaled / step_size[None, :, :, None]).reshape(proj_grads.shape)
    return (update, new_first, new_second)


def solution(mesh):
    in_specs = (
        P("dp", "tensor"),
        P("dp", "tensor"),
        P("dp", None, "tensor"),
        P("dp", "tensor"),
        P("dp", "tensor"),
        P("dp", "tensor"),
        P(),
        P(),
        P(("tensor", "dp"), None, None),
        P(),
    )
    out_specs = (P(("tensor", "dp"), None, None), P(("tensor", "dp"), None, None), P())
    return jax.shard_map(
        per_device, mesh=mesh, in_specs=in_specs, out_specs=out_specs, check_vma=False
    )
```
